128 devices in a mesh: dp: 1, col: 2 (over core), row: 64 (over z, y, x).
Axes of the slice: x: 4, y: 4, z: 4, core: 2. Of those that a mesh axis runs over, the one named last changes fastest.
Arguments:
- images: bfloat16 [16, 512, 256, 256], P('dp', 'row', 'col')
- w_down1: bfloat16 [3, 3, 256, 512], replicated
- b_down1: float32 [512], replicated
- w_refine1: bfloat16 [3, 3, 512, 512], replicated
- b_refine1: float32 [512], replicated
- w_down2: bfloat16 [3, 3, 512, 1024], replicated
- b_down2: float32 [1024], replicated
- w_refine2: bfloat16 [3, 3, 1024, 1024], replicated
- b_refine2: float32 [1024], replicated
- w_down3: bfloat16 [3, 3, 1024, 2048], replicated
- b_down3: float32 [2048], replicated
- w_refine3: bfloat16 [3, 3, 2048, 2048], replicated
- b_refine3: float32 [2048], replicated
Outputs:
- output: bfloat16 [16, 64, 32, 2048], P('dp', 'row', 'col')
All inputs are finite; a program needn't handle non-finite values.
Results may differ from the reference program's by a relative error of at most 0.00847578.
Values are sent between devices in bfloat16 or wider.
A program may use at most 1 GiB of HBM per device.

```python
import jax
import jax.numpy as jnp
from jax import lax

IMAGES = 16
HEIGHT = 512
WIDTH = 256
CH_IN = 256
CH_ONE = 512
CH_TWO = 1024
CH_THREE = 2048


def setup_inputs(seed: int = 0, part: int = 0) -> dict:
    base_key = jax.random.key(seed)
    key_list = jax.random.split(base_key, 13)
    image_key = jax.random.fold_in(key_list[0], part)
    pixels = jax.random.normal(image_key, (IMAGES, HEIGHT, WIDTH, CH_IN), jnp.float32)
    inputs = {"images": pixels.astype(jnp.bfloat16)}
    widths = (CH_IN, CH_ONE, CH_TWO, CH_THREE)
    for stage_idx in range(3):
        c_prev = widths[stage_idx]
        c_next = widths[stage_idx + 1]
        name_end = str(stage_idx + 1)
        down_draw = jax.random.normal(key_list[4 * stage_idx + 1], (3, 3, c_prev, c_next), jnp.float32)
        inputs["w_down" + name_end] = (down_draw * (2.0 / (9 * c_prev)) ** 0.5).astype(jnp.bfloat16)
        inputs["b_down" + name_end] = 0.4 * jax.random.normal(key_list[4 * stage_idx + 2], (c_next,), jnp.float32)
        refine_draw = jax.random.normal(key_list[4 * stage_idx + 3], (3, 3, c_next, c_next), jnp.float32)
        inputs["w_refine" + name_end] = (refine_draw * (2.0 / (9 * c_next)) ** 0.5).astype(jnp.bfloat16)
        inputs["b_refine" + name_end] = 0.4 * jax.random.normal(key_list[4 * stage_idx + 4], (c_next,), jnp.float32)
    return inputs


def conv_layer(feature, weight, bias_vec, stride):
    summed = lax.conv_general_dilated(feature.astype(jnp.float32), weight.astype(jnp.float32), (stride, stride), ((1, 1), (1, 1)), dimension_numbers=("NHWC", "HWIO", "NHWC"))
    return jnp.maximum(summed + bias_vec, 0.0).astype(jnp.bfloat16)


def reference(images, w_down1, b_down1, w_refine1, b_refine1, w_down2, b_down2, w_refine2, b_refine2, w_down3, b_down3, w_refine3, b_refine3):
    stages = ((w_down1, b_down1, w_refine1, b_refine1), (w_down2, b_down2, w_refine2, b_refine2), (w_down3, b_down3, w_refine3, b_refine3))

    def encode_one(single_image):
        feature = single_image[None]
        for w_down, b_down, w_refine, b_refine in stages:
            feature = conv_layer(feature, w_down, b_down, 2)
            feature = conv_layer(feature, w_refine, b_refine, 1)
        return feature[0]

    return lax.map(encode_one, images)
```

```python
import jax
import jax.numpy as jnp
from jax import lax
from jax.experimental import pallas as pl
from jax.experimental.pallas import tpu as pltpu
from jax.sharding import PartitionSpec as P

MESH = pl.DeviceIdType.MESH
BF16 = jnp.bfloat16
F32 = jnp.float32
VM = pltpu.VMEM
SEM = pltpu.SemaphoreType.DMA
ANY_SPEC = pl.BlockSpec(memory_space=pl.ANY)
VM_SPEC = pl.BlockSpec(memory_space=VM)
PARAMS = pltpu.CompilerParams(has_side_effects=True, vmem_limit_bytes=63 * 2**20)


def loop(count, fn):
    def body(step, carry):
        fn(step)
        return carry

    lax.fori_loop(0, count, body, 0)


def down_one_kernel(row_size, img_hbm, w_ref, b_ref, out_hbm, inb, halo, colb, corn, frow, xbuf, ybuf, in_sem, halo_send, halo_recv, col_sem, corn_sem, y_send, y_recv, self_sem):
    col = lax.axis_index("col")
    row = lax.axis_index("row")
    x = lax.rem(row, 4)
    base_row = row - x

    def image_of(step, xpos):
        group = lax.rem(xpos + 6 - lax.rem(step, 4), 4)
        return 4 * group + 2 * (step // 4)

    def load(step):
        slot = lax.rem(step, 2)
        return pltpu.make_async_copy(img_hbm.at[pl.ds(image_of(step, x), 2)], inb.at[slot], in_sem.at[slot])

    def halo_copy(step):
        first = image_of(step, lax.rem(x + 1, 4))
        return pltpu.make_async_remote_copy(img_hbm.at[pl.ds(first, 2), 7], halo.at[step], halo_send.at[step], halo_recv.at[step], device_id={"row": row + 1}, device_id_type=MESH)

    def col_copy():
        return pltpu.make_async_remote_copy(img_hbm.at[:, :, pl.ds(112, 16)], colb, col_sem.at[0], col_sem.at[1], device_id={"col": 1}, device_id_type=MESH)

    def corn_copy():
        return pltpu.make_async_remote_copy(img_hbm.at[:, 7, pl.ds(112, 16)], corn, corn_sem.at[0], corn_sem.at[1], device_id={"col": 1, "row": row + 1}, device_id_type=MESH)

    load(0).start()

    @pl.when(col == 0)
    def _():
        col_copy().start()

    @pl.when(row < row_size - 1)
    def _():
        @pl.when(col == 0)
        def _():
            corn_copy().start()

        def body(step):
            halo_copy(step).start()

        loop(8, body)

    @pl.when(col == 0)
    def _():
        colb[...] = jnp.zeros_like(colb)

    @pl.when(jnp.logical_or(col == 0, row == 0))
    def _():
        corn[...] = jnp.zeros_like(corn)

    @pl.when(row == 0)
    def _():
        halo[...] = jnp.zeros_like(halo)

    @pl.when(col == 1)
    def _():
        col_copy().wait_recv()

        @pl.when(row > 0)
        def _():
            corn_copy().wait_recv()

    def taps(i, q, left, line):
        for h in range(2):
            lanes = slice(128 * h, 128 * h + 128)
            frow[h, 0:16] = left[:, lanes].astype(F32)
            frow[h, 16:144] = line[:, lanes].astype(F32)
        for t in range(3):
            for h in range(2):
                xbuf[i, q, :, 256 * t + 128 * h : 256 * t + 128 * h + 128] = frow[h, pl.ds(15 + t, 64, stride=2)].astype(BF16)

    def y_copy(step, i):
        half = step // 4
        group = lax.rem(x + 6 - lax.rem(step, 4), 4)
        dst = out_hbm.at[half, pl.ds(4 * x, 4), pl.ds(pl.multiple_of(64 * col, 64), 64)]
        return pltpu.make_async_remote_copy(ybuf.at[step, i], dst, y_send.at[step * 2 + i], y_recv.at[half * 8 + 2 * x + col], device_id={"col": i, "row": base_row + group}, device_id_type=MESH)

    def y_local(half):
        dst = out_hbm.at[half, pl.ds(4 * x, 4), pl.ds(pl.multiple_of(64 * col, 64), 64)]
        return pltpu.make_async_copy(ybuf.at[4 * half + 2, col], dst, self_sem.at[half])

    def main(step):
        slot = lax.rem(step, 2)
        first = image_of(step, x)

        @pl.when(step < 7)
        def _():
            load(step + 1).start()

        load(step).wait()

        @pl.when(row > 0)
        def _():
            halo_copy(step).wait_recv()

        for i in range(2):
            taps(i, 0, corn[first + i], halo[step, i])

            def line(q, i=i):
                taps(i, q + 1, colb[first + i, q], inb[slot, i, q])

            loop(8, line)
        acc = None
        for dy in range(3):
            lhs = jnp.concatenate([xbuf[i, 2 * o + dy] for i in range(2) for o in range(4)], axis=0)
            part = jnp.dot(lhs, w_ref[dy], preferred_element_type=F32)
            acc = part if acc is None else acc + part
        out = jnp.maximum(acc + b_ref[...], 0.0).astype(BF16)
        for i in range(2):
            for o in range(4):
                ybuf[step, i, o] = out[(4 * i + o) * 64 : (4 * i + o + 1) * 64]
        for i in range(2):
            here = jnp.logical_and(lax.rem(step, 4) == 2, col == i)

            @pl.when(here)
            def _():
                y_local(step // 4).start()

            @pl.when(jnp.logical_not(here))
            def _(i=i):
                y_copy(step, i).start()

    loop(8, main)

    def finish(step):
        for i in range(2):
            here = jnp.logical_and(lax.rem(step, 4) == 2, col == i)

            @pl.when(here)
            def _():
                y_local(step // 4).wait()

            @pl.when(jnp.logical_not(here))
            def _(i=i):
                y_copy(step, i).wait_send()

        half = step // 4
        src_x = lax.rem(step, 4)
        for i in range(2):
            @pl.when(jnp.logical_or(src_x != x, col != i))
            def _(i=i):
                dst = out_hbm.at[half, pl.ds(4 * src_x, 4), pl.ds(64 * i, 64)]
                pltpu.make_async_remote_copy(ybuf.at[0, 0], dst, y_send.at[0], y_recv.at[half * 8 + 2 * src_x + i], device_id={"col": i, "row": base_row + src_x}, device_id_type=MESH).wait_recv()

        @pl.when(row < row_size - 1)
        def _():
            halo_copy(step).wait_send()


    loop(8, finish)

    @pl.when(col == 0)
    def _():
        col_copy().wait_send()

        @pl.when(row < row_size - 1)
        def _():
            corn_copy().wait_send()


def down_one(row_size, images, w, b):
    def kernel(*refs):
        down_one_kernel(row_size, *refs)

    return pl.pallas_call(
        kernel,
        out_shape=jax.ShapeDtypeStruct((2, 16, 128, 512), BF16),
        in_specs=[ANY_SPEC, VM_SPEC, VM_SPEC],
        out_specs=ANY_SPEC,
        scratch_shapes=[
            VM((2, 2, 8, 128, 256), BF16),
            VM((8, 2, 128, 256), BF16),
            VM((16, 8, 16, 256), BF16),
            VM((16, 16, 256), BF16),
            VM((2, 144, 128), F32),
            VM((2, 9, 64, 768), BF16),
            VM((8, 2, 4, 64, 512), BF16),
            SEM((2,)),
            SEM((8,)),
            SEM((8,)),
            SEM((2,)),
            SEM((2,)),
            SEM((16,)),
            SEM((16,)),
            SEM((2,)),
        ],
        compiler_params=PARAMS,
        name="down_one",
    )(images, w.reshape(3, 768, 512), b.reshape(1, 512))


def shifted(value, by, width):
    size = value.shape[0]
    pos = lax.rem(lax.broadcasted_iota(jnp.int32, (size, 1), 0), width)
    edge = 0 if by == 1 else width - 1
    return jnp.where(pos == edge, 0.0, pltpu.roll(value, by % size, 0))


def split_columns(value, scratch, even_ref, odd_ref, index, lane, rows, width):
    half = width // 2
    for h in range(2):
        scratch[h] = value[:, 128 * h : 128 * h + 128]
        lanes = pl.ds(pl.multiple_of(lane + 128 * h, 128), 128)
        for ref, start in ((even_ref, 0), (odd_ref, 1)):
            part = scratch[h, pl.ds(start, rows * half, stride=2)].astype(BF16)
            ref[index[0], index[1], :, lanes] = part.reshape(rows, half, 128)


def middle_kernel(row_size, y1_hbm, w1_hbm, w2_hbm, w3_hbm, b1_ref, b2_ref, b3_ref, even2, odd2, y1v, w1, w2, w3, even1, odd1, y2v, scratch, w_sem, in_sem, ha_s, ha_r, hb_s, hb_r, hc_s, hc_r, hd_s, hd_r):
    row = lax.axis_index("row")
    has_up = row >= 4
    has_down = row < row_size - 4

    def remote(src, dst, send, recv, delta):
        return pltpu.make_async_remote_copy(src, dst, send, recv, device_id={"row": row + delta}, device_id_type=MESH)

    def halo1_down(i):
        return remote(y1_hbm.at[i, 15], y1v.at[i, 0], ha_s.at[i], ha_r.at[i], 4)

    def halo1_up(i):
        return remote(y1_hbm.at[i, 0], y1v.at[i, 17], ha_s.at[2 + i], ha_r.at[2 + i], -4)

    def halo2(i, which):
        ref = (even1, odd1)[which]
        return remote(ref.at[i, 16], ref.at[i, 0], hb_s.at[2 * i + which], hb_r.at[2 * i + which], 4)

    def halo3_down(i):
        return remote(y2v.at[i, 8], y2v.at[i, 0], hc_s.at[i], hc_r.at[i], 4)

    def halo3_up(i):
        return remote(y2v.at[i, 1], y2v.at[i, 9], hc_s.at[2 + i], hc_r.at[2 + i], -4)

    def halo4(i, which):
        ref = (even2, odd2)[which]
        return remote(ref.at[i, 8], ref.at[i, 0], hd_s.at[2 * i + which], hd_r.at[2 * i + which], 4)

    loads = [pltpu.make_async_copy(y1_hbm.at[i], y1v.at[i, pl.ds(1, 16)], in_sem.at[i]) for i in range(2)]
    weights = [pltpu.make_async_copy(src, dst, w_sem.at[n]) for n, (src, dst) in enumerate(((w1_hbm, w1), (w2_hbm, w2), (w3_hbm, w3)))]

    @pl.when(has_down)
    def _():
        for i in range(2):
            halo1_down(i).start()

    @pl.when(has_up)
    def _():
        for i in range(2):
            halo1_up(i).start()

    weights[0].start()
    for i in range(2):
        loads[i].start()

    @pl.when(jnp.logical_not(has_up))
    def _():
        for i in range(2):
            for ref in (y1v, even1, odd1, y2v, even2, odd2):
                ref[i, 0] = jnp.zeros(ref.shape[2:], BF16)

    @pl.when(jnp.logical_not(has_down))
    def _():
        for i in range(2):
            y1v[i, 17] = jnp.zeros(y1v.shape[2:], BF16)
            y2v[i, 9] = jnp.zeros(y2v.shape[2:], BF16)

    for i in range(2):
        loads[i].wait()
    weights[0].wait()

    def refine_block(src, i, first, rows, w, lanes):
        width = src.shape[2]
        m = rows * width
        lhs = jnp.concatenate([src[i, pl.ds(first + dy, rows)].reshape(m, -1) for dy in range(3)], axis=1)
        parts = []
        for dx in range(3):
            rhs = jnp.concatenate([w[dy, dx, :, lanes] for dy in range(3)], axis=0)
            parts.append(jnp.dot(lhs, rhs, preferred_element_type=F32))
        return parts[1] + shifted(parts[0], 1, width) + shifted(parts[2], -1, width)

    def stage_r1(step):
        i = lax.rem(step, 2)
        block = lax.rem(1 + step // 2, 4)
        for n in (1, 2):
            @pl.when(step == n)
            def _(n=n):
                weights[n].start()

        @pl.when(step == 4)
        def _():
            @pl.when(has_down)
            def _():
                for k in range(2):
                    halo1_up(k).wait_recv()

            @pl.when(has_up)
            def _():
                for k in range(2):
                    halo1_down(k).wait_recv()

        def chunk(n):
            lanes = pl.ds(pl.multiple_of(n * 256, 256), 256)
            out = refine_block(y1v, i, 4 * block, 4, w1, lanes)
            out = jnp.maximum(out + b1_ref[:, lanes], 0.0)
            split_columns(out, scratch, even1, odd1, (i, pl.ds(1 + 4 * block, 4)), n * 256, 4, 128)

        loop(2, chunk)

        @pl.when(jnp.logical_and(has_down, block == 3))
        def _():
            for which in range(2):
                halo2(i, which).start()


    loop(8, stage_r1)
    weights[1].wait()

    def stage_d2(i):
        @pl.when(has_up)
        def _():
            for which in range(2):
                halo2(i, which).wait_recv()

        def chunk(n):
            lanes = pl.ds(pl.multiple_of(n * 256, 256), 256)

            def gather(ref):
                return [jnp.concatenate([ref[i, 2 * o + dy] for o in range(8)], axis=0) for dy in range(3)]

            odd = gather(odd1)
            both = jnp.concatenate(gather(even1) + odd, axis=1)
            rhs = jnp.concatenate([w2[dy, dx, :, lanes] for dx in (1, 2) for dy in range(3)], axis=0)
            left = jnp.concatenate([w2[dy, 0, :, lanes] for dy in range(3)], axis=0)
            out = jnp.dot(both, rhs, preferred_element_type=F32)
            out = out + shifted(jnp.dot(jnp.concatenate(odd, axis=1), left, preferred_element_type=F32), 1, 64)
            out = jnp.maximum(out + b2_ref[:, lanes], 0.0).astype(BF16)
            y2v[i, 1:9, :, lanes] = out.reshape(8, 64, 256)

        loop(4, chunk)

        @pl.when(has_down)
        def _():
            halo3_down(i).start()

        @pl.when(has_up)
        def _():
            halo3_up(i).start()


    loop(2, stage_d2)
    weights[2].wait()

    def stage_r2(i):
        @pl.when(has_up)
        def _():
            halo3_down(i).wait_recv()

        @pl.when(has_down)
        def _():
            halo3_up(i).wait_recv()

        def chunk(n):
            lanes = pl.ds(pl.multiple_of(n * 256, 256), 256)
            out = refine_block(y2v, i, 0, 8, w3, lanes)
            out = jnp.maximum(out + b3_ref[:, lanes], 0.0)
            split_columns(out, scratch, even2, odd2, (i, pl.ds(1, 8)), n * 256, 8, 64)

        loop(4, chunk)

        @pl.when(has_down)
        def _():
            for which in range(2):
                halo4(i, which).start()


    loop(2, stage_r2)

    @pl.when(has_down)
    def _():
        for i in range(2):
            halo1_down(i).wait_send()
            halo3_down(i).wait_send()
            for which in range(2):
                halo2(i, which).wait_send()
                halo4(i, which).wait_send()

    @pl.when(has_up)
    def _():
        for i in range(2):
            halo1_up(i).wait_send()
            halo3_up(i).wait_send()
            for which in range(2):
                halo4(i, which).wait_recv()


def middle(row_size, y1, w1, w2, w3, b1, b2, b3):
    def kernel(*refs):
        middle_kernel(row_size, *refs)

    return pl.pallas_call(
        kernel,
        out_shape=[jax.ShapeDtypeStruct((2, 9, 32, 1024), BF16)] * 2,
        in_specs=[ANY_SPEC] * 4 + [VM_SPEC] * 3,
        out_specs=[VM_SPEC] * 2,
        scratch_shapes=[
            VM((2, 18, 128, 512), BF16),
            VM((3, 3, 512, 512), BF16),
            VM((3, 3, 512, 1024), BF16),
            VM((3, 3, 1024, 1024), BF16),
            VM((2, 17, 64, 512), BF16),
            VM((2, 17, 64, 512), BF16),
            VM((2, 10, 64, 1024), BF16),
            VM((2, 512, 128), F32),
            SEM((3,)),
            SEM((2,)),
        ]
        + [SEM((4,))] * 8,
        compiler_params=PARAMS,
        name="middle",
    )(y1, w1, w2, w3, b1.reshape(1, -1), b2.reshape(1, -1), b3.reshape(1, -1))


RING = 4
WIDE = 512


def last_kernel(row_size, even2, odd2, w1_hbm, w2_hbm, b1_ref, b2_ref, out_hbm, w1, w2, y3v, obuf, lhs1, acc, w1_sem, w2_sem, up_s, up_r, down_s, down_r, o_s, o_r, self_sem):
    col = lax.axis_index("col")
    row = lax.axis_index("row")
    x = lax.rem(row, 4)
    base_row = row - x
    has_up = row >= 4
    has_down = row < row_size - 4
    total = 3 * (2048 // WIDE)

    def lanes_of(n):
        return pl.ds(pl.multiple_of(n * WIDE, WIDE), WIDE)

    def load(t, src, dst, sems):
        slot = lax.rem(t, RING)
        return pltpu.make_async_copy(src.at[:, lax.rem(t + 1, 3), :, lanes_of(t // 3)], dst.at[slot], sems.at[slot])

    def load1(t):
        return load(t, w1_hbm, w1, w1_sem)

    def load2(t):
        return load(t, w2_hbm, w2, w2_sem)

    def halo_up(n):
        return pltpu.make_async_remote_copy(y3v.at[:, 1, :, lanes_of(n)], y3v.at[:, 5, :, lanes_of(n)], up_s.at[n], up_r.at[n], device_id={"row": row - 4}, device_id_type=MESH)

    def halo_down(n):
        return pltpu.make_async_remote_copy(y3v.at[:, 4, :, lanes_of(n)], y3v.at[:, 0, :, lanes_of(n)], down_s.at[n], down_r.at[n], device_id={"row": row + 4}, device_id_type=MESH)

    def out_copy(n, xd, cd):
        dst = out_hbm.at[x, :, col, :, lanes_of(n)]
        return pltpu.make_async_remote_copy(obuf.at[n, :, xd, pl.ds(16 * cd, 16)], dst, o_s.at[n, 2 * xd + cd], o_r.at[n, 2 * x + col], device_id={"col": cd, "row": base_row + xd}, device_id_type=MESH)

    def out_recv(n, xs, cs):
        dst = out_hbm.at[xs, :, cs, :, lanes_of(n)]
        return pltpu.make_async_remote_copy(obuf.at[n, :, xs, pl.ds(16 * cs, 16)], dst, o_s.at[n, 2 * xs + cs], o_r.at[n, 2 * xs + cs], device_id={"col": cs, "row": base_row + xs}, device_id_type=MESH)

    def out_self(n):
        dst = out_hbm.at[x, :, col, :, lanes_of(n)]
        return pltpu.make_async_copy(obuf.at[n, :, x, pl.ds(pl.multiple_of(16 * col, 16), 16)], dst, self_sem.at[n])

    for t in range(RING - 1):
        load1(t).start()

    @pl.when(jnp.logical_not(has_up))
    def _():
        y3v[:, 0] = jnp.zeros((2, 32, 2048), BF16)

    @pl.when(jnp.logical_not(has_down))
    def _():
        y3v[:, 5] = jnp.zeros((2, 32, 2048), BF16)

    for k, ref in enumerate((even2, odd2)):
        for dy in range(3):
            for i in range(2):
                for o in range(4):
                    first = 32 * (4 * i + o)
                    lhs1[k, first : first + 32, 1024 * dy : 1024 * dy + 1024] = ref[i, 2 * o + dy]

    def stage_d3(t):
        load1(t).wait()
        ahead = t + RING - 1

        @pl.when(ahead < total)
        def _():
            load1(ahead).start()

        @pl.when(ahead >= total)
        def _():
            load2(ahead - total).start()

        j = lax.rem(t, 3)
        n = t // 3
        acc[j] = jnp.dot(lhs1[(j + 1) // 2], w1[lax.rem(t, RING)].reshape(3072, WIDE), preferred_element_type=F32)

        @pl.when(j == 2)
        def _():
            out = acc[0] + acc[1] + shifted(acc[2], 1, 32)
            out = jnp.maximum(out + b1_ref[:, lanes_of(n)], 0.0).astype(BF16)
            y3v[:, 1:5, :, lanes_of(n)] = out.reshape(2, 4, 32, WIDE)

            @pl.when(has_up)
            def _():
                halo_up(n).start()

            @pl.when(has_down)
            def _():
                halo_down(n).start()

    loop(total, stage_d3)

    def halo_wait(n):
        @pl.when(has_down)
        def _():
            halo_up(n).wait_recv()

        @pl.when(has_up)
        def _():
            halo_down(n).wait_recv()

    loop(total // 3, halo_wait)

    def stage_r3(t):
        load2(t).wait()
        ahead = t + RING - 1

        @pl.when(ahead < total)
        def _():
            load2(ahead).start()

        j = lax.rem(t, 3)
        n = t // 3
        lhs = jnp.concatenate([y3v[:, dy : dy + 4].reshape(256, 2048) for dy in range(3)], axis=1)
        acc[j] = jnp.dot(lhs, w2[lax.rem(t, RING)].reshape(6144, WIDE), preferred_element_type=F32)

        @pl.when(j == 2)
        def _():
            out = acc[0] + shifted(acc[1], -1, 32) + shifted(acc[2], 1, 32)
            out = jnp.maximum(out + b2_ref[:, lanes_of(n)], 0.0).astype(BF16)
            obuf[n] = out.reshape(2, 4, 32, WIDE)
            for xd in range(4):
                for cd in range(2):
                    here = jnp.logical_and(x == xd, col == cd)

                    @pl.when(here)
                    def _():
                        out_self(n).start()

                    @pl.when(jnp.logical_not(here))
                    def _(xd=xd, cd=cd):
                        out_copy(n, xd, cd).start()

    loop(total, stage_r3)

    def finish(n):
        out_self(n).wait()
        for xd in range(4):
            for cd in range(2):
                @pl.when(jnp.logical_or(x != xd, col != cd))
                def _(xd=xd, cd=cd):
                    out_copy(n, xd, cd).wait_send()
                    out_recv(n, xd, cd).wait_recv()

        @pl.when(has_up)
        def _():
            halo_up(n).wait_send()

        @pl.when(has_down)
        def _():
            halo_down(n).wait_send()

    loop(total // 3, finish)


def last(row_size, even2, odd2, w1, w2, b1, b2):
    def kernel(*refs):
        last_kernel(row_size, *refs)

    return pl.pallas_call(
        kernel,
        out_shape=jax.ShapeDtypeStruct((4, 2, 2, 16, 2048), BF16),
        in_specs=[VM_SPEC, VM_SPEC, ANY_SPEC, ANY_SPEC, VM_SPEC, VM_SPEC],
        out_specs=ANY_SPEC,
        scratch_shapes=[
            VM((RING, 3, 1024, WIDE), BF16),
            VM((RING, 3, 2048, WIDE), BF16),
            VM((2, 6, 32, 2048), BF16),
            VM((4, 2, 4, 32, WIDE), BF16),
            VM((2, 256, 3072), BF16),
            VM((3, 256, WIDE), F32),
        ]
        + [SEM((RING,))] * 6
        + [SEM((RING, 8))] * 2
        + [SEM((RING,))],
        compiler_params=PARAMS,
        name="last",
    )(even2, odd2, w1, w2, b1.reshape(1, -1), b2.reshape(1, -1))


def solution(mesh):
    row_size = mesh.shape["row"]

    def local_encoder(images, w_down1, b_down1, w_refine1, b_refine1, w_down2, b_down2, w_refine2, b_refine2, w_down3, b_down3, w_refine3, b_refine3):
        y = down_one(row_size, images, w_down1, b_down1)
        even, odd = middle(row_size, y, w_refine1, w_down2, w_refine2, b_refine1, b_down2, b_refine2)
        out = last(row_size, even, odd, w_down3, w_refine3, b_down3, b_refine3)
        return out.reshape(16, 1, 16, 2048)

    tile_spec = P("dp", "row", "col")
    return jax.shard_map(local_encoder, mesh=mesh, in_specs=(tile_spec,) + (P(),) * 12, out_specs=tile_spec, check_vma=False)
```

```python
import jax
import jax.numpy as jnp
from jax import lax
from jax.experimental import pallas as pl
from jax.experimental.pallas import tpu as pltpu
from jax.sharding import PartitionSpec as P

MESH = pl.DeviceIdType.MESH
BF16 = jnp.bfloat16
F32 = jnp.float32
VM = pltpu.VMEM
SEM = pltpu.SemaphoreType.DMA
ANY_SPEC = pl.BlockSpec(memory_space=pl.ANY)
VM_SPEC = pl.BlockSpec(memory_space=VM)
PARAMS = pltpu.CompilerParams(has_side_effects=True, vmem_limit_bytes=63 * 2**20)


def loop(count, fn):
    def body(step, carry):
        fn(step)
        return carry

    lax.fori_loop(0, count, body, 0)


def shifted(value, by, width):
    size = value.shape[0]
    pos = lax.rem(lax.broadcasted_iota(jnp.int32, (size, 1), 0), width)
    edge = 0 if by == 1 else width - 1
    return jnp.where(pos == edge, 0.0, pltpu.roll(value, by % size, 0))


def split_columns(value, scratch, even_ref, odd_ref, index, lane, rows, width):
    half = width // 2
    for h in range(2):
        scratch[h] = value[:, 128 * h : 128 * h + 128]
        lanes = pl.ds(pl.multiple_of(lane + 128 * h, 128), 128)
        for ref, start in ((even_ref, 0), (odd_ref, 1)):
            part = scratch[h, pl.ds(start, rows * half, stride=2)].astype(BF16)
            ref[index[0], index[1], :, lanes] = part.reshape(rows, half, 128)


def front_kernel(row_size, img_hbm, w0_ref, b0_ref, w1_hbm, w2_hbm, w3_hbm, b1_ref, b2_ref, b3_ref, even2, odd2, inb, halo, colb, corn, frow, xbuf, ybuf, y1v, w1, w2, w3, even1, odd1, y2v, scratch, in_sem, halo_send, halo_recv, col_sem, corn_sem, y_send, y_recv, self_sem, w_sem, ha_s, ha_r, hb_s, hb_r, hc_s, hc_r, hd_s, hd_r):
    col = lax.axis_index("col")
    row = lax.axis_index("row")
    x = lax.rem(row, 4)
    base_row = row - x
    has_up = row >= 4
    has_down = row < row_size - 4
    sends_row = row < row_size - 1
    weights = [pltpu.make_async_copy(src, dst, w_sem.at[n]) for n, (src, dst) in enumerate(((w1_hbm, w1), (w2_hbm, w2), (w3_hbm, w3)))]

    def group_of(step, xpos):
        return lax.rem(xpos + 6 - lax.rem(step, 4), 4)

    def image_of(step, xpos):
        return 4 * group_of(step, xpos) + 2 * (step // 4)

    def load(step):
        slot = lax.rem(step, 2)
        return pltpu.make_async_copy(img_hbm.at[pl.ds(image_of(step, x), 2)], inb.at[slot], in_sem.at[slot])

    def halo_copy(step):
        first = image_of(step, lax.rem(x + 1, 4))
        return pltpu.make_async_remote_copy(img_hbm.at[pl.ds(first, 2), 7], halo.at[step], halo_send.at[step], halo_recv.at[step], device_id={"row": row + 1}, device_id_type=MESH)

    def col_copy():
        return pltpu.make_async_remote_copy(img_hbm.at[:, :, pl.ds(112, 16)], colb, col_sem.at[0], col_sem.at[1], device_id={"col": 1}, device_id_type=MESH)

    def corn_copy():
        return pltpu.make_async_remote_copy(img_hbm.at[:, 7, pl.ds(112, 16)], corn, corn_sem.at[0], corn_sem.at[1], device_id={"col": 1, "row": row + 1}, device_id_type=MESH)

    def y_place(half, xs, cs):
        return y1v.at[half, pl.ds(1 + 4 * xs, 4), pl.ds(pl.multiple_of(64 * cs, 64), 64)]

    def y_copy(step, i):
        half = step // 4
        return pltpu.make_async_remote_copy(ybuf.at[step, i], y_place(half, x, col), y_send.at[step * 2 + i], y_recv.at[half * 8 + 2 * x + col], device_id={"col": i, "row": base_row + group_of(step, x)}, device_id_type=MESH)

    def y_local(half):
        return pltpu.make_async_copy(ybuf.at[4 * half + 2, col], y_place(half, x, col), self_sem.at[half])

    def ring(src, dst, send, recv, delta):
        return pltpu.make_async_remote_copy(src, dst, send, recv, device_id={"row": row + delta}, device_id_type=MESH)

    def halo1_down(i):
        return ring(y1v.at[i, 16], y1v.at[i, 0], ha_s.at[i], ha_r.at[i], 4)

    def halo1_up(i):
        return ring(y1v.at[i, 1], y1v.at[i, 17], ha_s.at[2 + i], ha_r.at[2 + i], -4)

    def halo2(i, which):
        ref = (even1, odd1)[which]
        return ring(ref.at[i, 16], ref.at[i, 0], hb_s.at[2 * i + which], hb_r.at[2 * i + which], 4)

    def halo3_down(i):
        return ring(y2v.at[i, 8], y2v.at[i, 0], hc_s.at[i], hc_r.at[i], 4)

    def halo3_up(i):
        return ring(y2v.at[i, 1], y2v.at[i, 9], hc_s.at[2 + i], hc_r.at[2 + i], -4)

    def halo4(i, which):
        ref = (even2, odd2)[which]
        return ring(ref.at[i, 8], ref.at[i, 0], hd_s.at[2 * i + which], hd_r.at[2 * i + which], 4)

    load(0).start()

    @pl.when(col == 0)
    def _():
        col_copy().start()

    @pl.when(sends_row)
    def _():
        @pl.when(col == 0)
        def _():
            corn_copy().start()

        def body(step):
            halo_copy(step).start()

        loop(8, body)

    @pl.when(col == 0)
    def _():
        colb[...] = jnp.zeros_like(colb)

    @pl.when(jnp.logical_or(col == 0, row == 0))
    def _():
        corn[...] = jnp.zeros_like(corn)

    @pl.when(row == 0)
    def _():
        halo[...] = jnp.zeros_like(halo)

    @pl.when(jnp.logical_not(has_up))
    def _():
        for i in range(2):
            for ref in (y1v, even1, odd1, y2v, even2, odd2):
                ref[i, 0] = jnp.zeros(ref.shape[2:], BF16)

    @pl.when(jnp.logical_not(has_down))
    def _():
        for i in range(2):
            y1v[i, 17] = jnp.zeros(y1v.shape[2:], BF16)
            y2v[i, 9] = jnp.zeros(y2v.shape[2:], BF16)

    @pl.when(col == 1)
    def _():
        col_copy().wait_recv()

        @pl.when(row > 0)
        def _():
            corn_copy().wait_recv()

    def taps(i, q, left, line):
        for h in range(2):
            lanes = slice(128 * h, 128 * h + 128)
            frow[h, 0:16] = left[:, lanes].astype(F32)
            frow[h, 16:144] = line[:, lanes].astype(F32)
        for t in range(3):
            for h in range(2):
                xbuf[i, q, :, 256 * t + 128 * h : 256 * t + 128 * h + 128] = frow[h, pl.ds(15 + t, 64, stride=2)].astype(BF16)

    def is_local(step, i):
        return jnp.logical_and(lax.rem(step, 4) == 2, col == i)

    def stage_d1(step):
        slot = lax.rem(step, 2)
        first = image_of(step, x)

        @pl.when(step < 7)
        def _():
            load(step + 1).start()

        for n in range(3):
            @pl.when(step == n + 1)
            def _(n=n):
                weights[n].start()

        load(step).wait()

        @pl.when(row > 0)
        def _():
            halo_copy(step).wait_recv()

        for i in range(2):
            taps(i, 0, corn[first + i], halo[step, i])

            def line(q, i=i):
                taps(i, q + 1, colb[first + i, q], inb[slot, i, q])

            loop(8, line)
        acc = None
        for dy in range(3):
            lhs = jnp.concatenate([xbuf[i, 2 * o + dy] for i in range(2) for o in range(4)], axis=0)
            part = jnp.dot(lhs, w0_ref[dy], preferred_element_type=F32)
            acc = part if acc is None else acc + part
        out = jnp.maximum(acc + b0_ref[...], 0.0).astype(BF16)
        ybuf[step] = out.reshape(2, 4, 64, 512)
        for i in range(2):
            here = is_local(step, i)

            @pl.when(here)
            def _():
                y_local(step // 4).start()

            @pl.when(jnp.logical_not(here))
            def _(i=i):
                y_copy(step, i).start()

    loop(8, stage_d1)

    def refine_block(src, i, first, rows, w, lanes):
        width = src.shape[2]
        m = rows * width
        lhs = jnp.concatenate([src[i, pl.ds(first + dy, rows)].reshape(m, -1) for dy in range(3)], axis=1)
        parts = []
        for dx in range(3):
            rhs = jnp.concatenate([w[dy, dx, :, lanes] for dy in range(3)], axis=0)
            parts.append(jnp.dot(lhs, rhs, preferred_element_type=F32))
        return parts[1] + shifted(parts[0], 1, width) + shifted(parts[2], -1, width)

    def lanes_of(n):
        return pl.ds(pl.multiple_of(n * 256, 256), 256)

    def stage_r1(i):
        def piece(step):
            block = lax.rem(1 + step, 4)

            @pl.when(block == 3)
            def _():
                @pl.when(has_down)
                def _():
                    halo1_up(i).wait_recv()

                @pl.when(has_up)
                def _():
                    halo1_down(i).wait_recv()

            def chunk(n):
                lanes = lanes_of(n)
                out = refine_block(y1v, i, 4 * block, 4, w1, lanes)
                out = jnp.maximum(out + b1_ref[:, lanes], 0.0)
                split_columns(out, scratch, even1, odd1, (i, pl.ds(1 + 4 * block, 4)), n * 256, 4, 128)

            loop(2, chunk)

            @pl.when(jnp.logical_and(has_down, block == 3))
            def _():
                for which in range(2):
                    halo2(i, which).start()

        loop(4, piece)

    def stage_d2(i):
        @pl.when(has_up)
        def _():
            for which in range(2):
                halo2(i, which).wait_recv()

        def chunk(n):
            lanes = lanes_of(n)

            def gather(ref):
                return [jnp.concatenate([ref[i, 2 * o + dy] for o in range(8)], axis=0) for dy in range(3)]

            odd = gather(odd1)
            both = jnp.concatenate(gather(even1) + odd, axis=1)
            rhs = jnp.concatenate([w2[dy, dx, :, lanes] for dx in (1, 2) for dy in range(3)], axis=0)
            left = jnp.concatenate([w2[dy, 0, :, lanes] for dy in range(3)], axis=0)
            out = jnp.dot(both, rhs, preferred_element_type=F32)
            out = out + shifted(jnp.dot(jnp.concatenate(odd, axis=1), left, preferred_element_type=F32), 1, 64)
            out = jnp.maximum(out + b2_ref[:, lanes], 0.0).astype(BF16)
            y2v[i, 1:9, :, lanes] = out.reshape(8, 64, 256)

        loop(4, chunk)

        @pl.when(has_down)
        def _():
            halo3_down(i).start()

        @pl.when(has_up)
        def _():
            halo3_up(i).start()

    def halo3_wait(i):
        @pl.when(has_up)
        def _():
            halo3_down(i).wait_recv()

        @pl.when(has_down)
        def _():
            halo3_up(i).wait_recv()

    def stage_r2(i, first, count):
        def chunk(step):
            n = first + step
            lanes = lanes_of(n)
            out = refine_block(y2v, i, 0, 8, w3, lanes)
            out = jnp.maximum(out + b3_ref[:, lanes], 0.0)
            split_columns(out, scratch, even2, odd2, (i, pl.ds(1, 8)), n * 256, 8, 64)

        loop(count, chunk)

    def halo4_start(i):
        @pl.when(has_down)
        def _():
            for which in range(2):
                halo4(i, which).start()

    def per_image(half):
        y_local(half).wait()
        for xs in range(4):
            for cs in range(2):
                @pl.when(jnp.logical_or(xs != x, cs != col))
                def _(xs=xs, cs=cs):
                    pltpu.make_async_remote_copy(ybuf.at[0, 0], y_place(half, xs, cs), y_send.at[0], y_recv.at[half * 8 + 2 * xs + cs], device_id={"col": cs, "row": base_row + xs}, device_id_type=MESH).wait_recv()

        @pl.when(has_down)
        def _():
            halo1_down(half).start()

        @pl.when(has_up)
        def _():
            halo1_up(half).start()

        @pl.when(half == 0)
        def _():
            weights[0].wait()

        stage_r1(half)

        @pl.when(half == 0)
        def _():
            weights[1].wait()

        stage_d2(half)

        @pl.when(half == 0)
        def _():
            halo3_wait(0)
            weights[2].wait()

        stage_r2(0, 2 * half, 2)

    loop(2, per_image)
    halo4_start(0)
    halo3_wait(1)
    stage_r2(1, 0, 4)
    halo4_start(1)

    def finish(step):
        for i in range(2):
            @pl.when(jnp.logical_not(is_local(step, i)))
            def _(i=i):
                y_copy(step, i).wait_send()

        @pl.when(sends_row)
        def _():
            halo_copy(step).wait_send()

    loop(8, finish)

    @pl.when(col == 0)
    def _():
        col_copy().wait_send()

        @pl.when(sends_row)
        def _():
            corn_copy().wait_send()

    @pl.when(has_down)
    def _():
        for i in range(2):
            halo1_down(i).wait_send()
            halo3_down(i).wait_send()
            for which in range(2):
                halo2(i, which).wait_send()
                halo4(i, which).wait_send()

    @pl.when(has_up)
    def _():
        for i in range(2):
            halo1_up(i).wait_send()
            halo3_up(i).wait_send()
            for which in range(2):
                halo4(i, which).wait_recv()


def front(row_size, images, w0, b0, w1, w2, w3, b1, b2, b3):
    def kernel(*refs):
        front_kernel(row_size, *refs)

    return pl.pallas_call(
        kernel,
        out_shape=[jax.ShapeDtypeStruct((2, 9, 32, 1024), BF16)] * 2,
        in_specs=[ANY_SPEC, VM_SPEC, VM_SPEC] + [ANY_SPEC] * 3 + [VM_SPEC] * 3,
        out_specs=[VM_SPEC] * 2,
        scratch_shapes=[
            VM((2, 2, 8, 128, 256), BF16),
            VM((8, 2, 128, 256), BF16),
            VM((16, 8, 16, 256), BF16),
            VM((16, 16, 256), BF16),
            VM((2, 144, 128), F32),
            VM((2, 9, 64, 768), BF16),
            VM((8, 2, 4, 64, 512), BF16),
            VM((2, 18, 128, 512), BF16),
            VM((3, 3, 512, 512), BF16),
            VM((3, 3, 512, 1024), BF16),
            VM((3, 3, 1024, 1024), BF16),
            VM((2, 17, 64, 512), BF16),
            VM((2, 17, 64, 512), BF16),
            VM((2, 10, 64, 1024), BF16),
            VM((2, 512, 128), F32),
        ]
        + [SEM((n,)) for n in (2, 8, 8, 2, 2, 16, 16, 2, 3)]
        + [SEM((4,))] * 8,
        compiler_params=PARAMS,
        name="front",
    )(images, w0.reshape(3, 768, 512), b0.reshape(1, 512), w1, w2, w3, b1.reshape(1, -1), b2.reshape(1, -1), b3.reshape(1, -1))


RING = 4
WIDE = 512


def last_kernel(row_size, even2, odd2, w1_hbm, w2_hbm, b1_ref, b2_ref, out_hbm, w1, w2, y3v, obuf, lhs1, acc, w1_sem, w2_sem, up_s, up_r, down_s, down_r, o_s, o_r, self_sem):
    col = lax.axis_index("col")
    row = lax.axis_index("row")
    x = lax.rem(row, 4)
    base_row = row - x
    has_up = row >= 4
    has_down = row < row_size - 4
    total = 3 * (2048 // WIDE)

    def lanes_of(n):
        return pl.ds(pl.multiple_of(n * WIDE, WIDE), WIDE)

    def load(t, src, dst, sems):
        slot = lax.rem(t, RING)
        return pltpu.make_async_copy(src.at[:, lax.rem(t + 1, 3), :, lanes_of(t // 3)], dst.at[slot], sems.at[slot])

    def load1(t):
        return load(t, w1_hbm, w1, w1_sem)

    def load2(t):
        return load(t, w2_hbm, w2, w2_sem)

    def halo_up(n):
        return pltpu.make_async_remote_copy(y3v.at[:, 1, :, lanes_of(n)], y3v.at[:, 5, :, lanes_of(n)], up_s.at[n], up_r.at[n], device_id={"row": row - 4}, device_id_type=MESH)

    def halo_down(n):
        return pltpu.make_async_remote_copy(y3v.at[:, 4, :, lanes_of(n)], y3v.at[:, 0, :, lanes_of(n)], down_s.at[n], down_r.at[n], device_id={"row": row + 4}, device_id_type=MESH)

    def out_copy(n, xd, cd):
        dst = out_hbm.at[x, :, col, :, lanes_of(n)]
        return pltpu.make_async_remote_copy(obuf.at[n, :, xd, pl.ds(16 * cd, 16)], dst, o_s.at[n, 2 * xd + cd], o_r.at[n, 2 * x + col], device_id={"col": cd, "row": base_row + xd}, device_id_type=MESH)

    def out_recv(n, xs, cs):
        dst = out_hbm.at[xs, :, cs, :, lanes_of(n)]
        return pltpu.make_async_remote_copy(obuf.at[n, :, xs, pl.ds(16 * cs, 16)], dst, o_s.at[n, 2 * xs + cs], o_r.at[n, 2 * xs + cs], device_id={"col": cs, "row": base_row + xs}, device_id_type=MESH)

    def out_self(n):
        dst = out_hbm.at[x, :, col, :, lanes_of(n)]
        return pltpu.make_async_copy(obuf.at[n, :, x, pl.ds(pl.multiple_of(16 * col, 16), 16)], dst, self_sem.at[n])

    for t in range(RING - 1):
        load1(t).start()

    @pl.when(jnp.logical_not(has_up))
    def _():
        y3v[:, 0] = jnp.zeros((2, 32, 2048), BF16)

    @pl.when(jnp.logical_not(has_down))
    def _():
        y3v[:, 5] = jnp.zeros((2, 32, 2048), BF16)

    for k, ref in enumerate((even2, odd2)):
        for dy in range(3):
            for i in range(2):
                for o in range(4):
                    first = 32 * (4 * i + o)
                    lhs1[k, first : first + 32, 1024 * dy : 1024 * dy + 1024] = ref[i, 2 * o + dy]

    def stage_d3(t):
        load1(t).wait()
        ahead = t + RING - 1

        @pl.when(ahead < total)
        def _():
            load1(ahead).start()

        @pl.when(ahead >= total)
        def _():
            load2(ahead - total).start()

        j = lax.rem(t, 3)
        n = t // 3
        acc[j] = jnp.dot(lhs1[(j + 1) // 2], w1[lax.rem(t, RING)].reshape(3072, WIDE), preferred_element_type=F32)

        @pl.when(j == 2)
        def _():
            out = acc[0] + acc[1] + shifted(acc[2], 1, 32)
            out = jnp.maximum(out + b1_ref[:, lanes_of(n)], 0.0).astype(BF16)
            y3v[:, 1:5, :, lanes_of(n)] = out.reshape(2, 4, 32, WIDE)

            @pl.when(has_up)
            def _():
                halo_up(n).start()

            @pl.when(has_down)
            def _():
                halo_down(n).start()

    loop(total, stage_d3)

    def halo_wait(n):
        @pl.when(has_down)
        def _():
            halo_up(n).wait_recv()

        @pl.when(has_up)
        def _():
            halo_down(n).wait_recv()

    loop(total // 3, halo_wait)

    def stage_r3(t):
        load2(t).wait()
        ahead = t + RING - 1

        @pl.when(ahead < total)
        def _():
            load2(ahead).start()

        j = lax.rem(t, 3)
        n = t // 3
        lhs = jnp.concatenate([y3v[:, dy : dy + 4].reshape(256, 2048) for dy in range(3)], axis=1)
        acc[j] = jnp.dot(lhs, w2[lax.rem(t, RING)].reshape(6144, WIDE), preferred_element_type=F32)

        @pl.when(j == 2)
        def _():
            out = acc[0] + shifted(acc[1], -1, 32) + shifted(acc[2], 1, 32)
            out = jnp.maximum(out + b2_ref[:, lanes_of(n)], 0.0).astype(BF16)
            obuf[n] = out.reshape(2, 4, 32, WIDE)
            for xd in range(4):
                for cd in range(2):
                    here = jnp.logical_and(x == xd, col == cd)

                    @pl.when(here)
                    def _():
                        out_self(n).start()

                    @pl.when(jnp.logical_not(here))
                    def _(xd=xd, cd=cd):
                        out_copy(n, xd, cd).start()

    loop(total, stage_r3)

    def finish(n):
        out_self(n).wait()
        for xd in range(4):
            for cd in range(2):
                @pl.when(jnp.logical_or(x != xd, col != cd))
                def _(xd=xd, cd=cd):
                    out_copy(n, xd, cd).wait_send()
                    out_recv(n, xd, cd).wait_recv()

        @pl.when(has_up)
        def _():
            halo_up(n).wait_send()

        @pl.when(has_down)
        def _():
            halo_down(n).wait_send()

    loop(total // 3, finish)


def last(row_size, even2, odd2, w1, w2, b1, b2):
    def kernel(*refs):
        last_kernel(row_size, *refs)

    return pl.pallas_call(
        kernel,
        out_shape=jax.ShapeDtypeStruct((4, 2, 2, 16, 2048), BF16),
        in_specs=[VM_SPEC, VM_SPEC, ANY_SPEC, ANY_SPEC, VM_SPEC, VM_SPEC],
        out_specs=ANY_SPEC,
        scratch_shapes=[
            VM((RING, 3, 1024, WIDE), BF16),
            VM((RING, 3, 2048, WIDE), BF16),
            VM((2, 6, 32, 2048), BF16),
            VM((4, 2, 4, 32, WIDE), BF16),
            VM((2, 256, 3072), BF16),
            VM((3, 256, WIDE), F32),
        ]
        + [SEM((RING,))] * 6
        + [SEM((RING, 8))] * 2
        + [SEM((RING,))],
        compiler_params=PARAMS,
        name="last",
    )(even2, odd2, w1, w2, b1.reshape(1, -1), b2.reshape(1, -1))


def solution(mesh):
    row_size = mesh.shape["row"]

    def local_encoder(images, w_down1, b_down1, w_refine1, b_refine1, w_down2, b_down2, w_refine2, b_refine2, w_down3, b_down3, w_refine3, b_refine3):
        even, odd = front(row_size, images, w_down1, b_down1, w_refine1, w_down2, w_refine2, b_refine1, b_down2, b_refine2)
        out = last(row_size, even, odd, w_down3, w_refine3, b_down3, b_refine3)
        return out.reshape(16, 1, 16, 2048)

    tile_spec = P("dp", "row", "col")
    return jax.shard_map(local_encoder, mesh=mesh, in_specs=(tile_spec,) + (P(),) * 12, out_specs=tile_spec, check_vma=False)
```

```python
import jax
import jax.numpy as jnp
from jax import lax
from jax.experimental import pallas as pl
from jax.experimental.pallas import tpu as pltpu
from jax.sharding import PartitionSpec as P

MESH = pl.DeviceIdType.MESH
BF16 = jnp.bfloat16
F32 = jnp.float32
WIDE = 512
TOP = 2048
MID = 1024
PART = 256
LANE = 128
HALF = 64
VM = pltpu.VMEM
SEM = pltpu.SemaphoreType.DMA
ANY_SPEC = pl.BlockSpec(memory_space=pl.ANY)
VM_SPEC = pl.BlockSpec(memory_space=VM)
PARAMS = pltpu.CompilerParams(has_side_effects=True, vmem_limit_bytes=67043328)


def loop(count, fn):
    def body(step, carry):
        fn(step)
        return carry

    lax.fori_loop(0, count, body, 0)


def shifted(value, by, width):
    size = value.shape[0]
    pos = lax.rem(lax.broadcasted_iota(jnp.int32, (size, 1), 0), width)
    edge = 0 if by == 1 else width - 1
    return jnp.where(pos == edge, 0.0, pltpu.roll(value, by % size, 0))


def split_columns(value, scratch, even_ref, odd_ref, index, lane, rows, width):
    half = width // 2
    for h in range(2):
        scratch[h, 0 : rows * width] = value[:, LANE * h : LANE * h + LANE]
        lanes = pl.ds(pl.multiple_of(lane + LANE * h, LANE), LANE)
        for ref, start in ((even_ref, 0), (odd_ref, 1)):
            part = scratch[h, pl.ds(start, rows * half, stride=2)].astype(BF16)
            ref[index[0], index[1], :, lanes] = part.reshape(rows, half, LANE)


def encoder_kernel(row_size, img_hbm, w0_ref, b0_ref, w1_hbm, w2_hbm, w3_hbm, w4_hbm, w5_hbm, b1_ref, b2_ref, b3_ref, b4_ref, b5_ref, out_hbm, inb, halo, colb, corn, frow, xbuf, ybuf, y1v, wbuf, eo1, y2v, scratch, eo2, y3v, acc, in_sem, halo_send, halo_recv, col_sem, corn_sem, y_send, y_recv, self_sem, w_sem, ha_s, ha_r, hb_s, hb_r, hc_s, hc_r, hd_s, hd_r, up_s, up_r, down_s, down_r, out_sem, w4_sem, w5_sem, o_s, o_r):
    col = lax.axis_index("col")
    row = lax.axis_index("row")
    x = lax.rem(row, 4)
    base_row = row - x
    has_up = row >= 4
    has_down = row < row_size - 4
    sends_row = row < row_size - 1
    total = 3 * (TOP // WIDE)

    def plane(src, part, first, count, n):
        return pltpu.make_async_copy(src.at[:, :, pl.ds(WIDE * part, WIDE)], wbuf.at[pl.ds(first, count)], w_sem.at[n])

    weights = [[plane(w1_hbm, 0, 0, 9, 0)], [plane(w2_hbm, k, 9 + 9 * k, 9, 1 + k) for k in range(2)], [plane(w3_hbm, k, 27 + 18 * k, 18, 3 + k) for k in range(2)]]

    def weights_start(n):
        for copy in weights[n]:
            copy.start()

    def weights_wait(n):
        for copy in weights[n]:
            copy.wait()

    def wide(n):
        return pl.ds(pl.multiple_of(n * WIDE, WIDE), WIDE)

    def load4(t):
        slot = lax.rem(t, 4)
        return [pltpu.make_async_copy(w4_hbm.at[dy, lax.rem(t + 1, 3), :, :, wide(t // 3)], wbuf.at[pl.ds(6 * slot + 2 * dy, 2)], w4_sem.at[slot, dy]) for dy in range(3)]

    def base5(t):
        return lax.rem(27 + 12 * lax.rem(t, 5), 63)

    def load5(t):
        return [pltpu.make_async_copy(w5_hbm.at[dy, lax.rem(t + 1, 3), :, :, wide(t // 3)], wbuf.at[pl.ds(base5(t) + 4 * dy, 4)], w5_sem.at[lax.rem(t, 5), dy]) for dy in range(3)]

    def start_all(copies):
        for copy in copies:
            copy.start()

    def wait_all(copies):
        for copy in copies:
            copy.wait()

    def group_of(step, xpos):
        turn = lax.rem(step, 4)
        turn = jnp.where(turn < 2, turn + col * (1 - 2 * turn), turn)
        return lax.rem(xpos + 6 - turn, 4)

    def image_of(step, xpos):
        return 4 * group_of(step, xpos) + 2 * (step // 4)

    def load(step):
        slot = lax.rem(step, 2)
        return pltpu.make_async_copy(img_hbm.at[pl.ds(image_of(step, x), 2)], inb.at[slot], in_sem.at[slot])

    def halo_copy(step):
        first = image_of(step, lax.rem(x + 1, 4))
        return pltpu.make_async_remote_copy(img_hbm.at[pl.ds(first, 2), 7], halo.at[step], halo_send.at[step], halo_recv.at[step], device_id={"row": row + 1}, device_id_type=MESH)

    def col_copy():
        return pltpu.make_async_remote_copy(img_hbm.at[:, :, pl.ds(120, 8)], colb, col_sem.at[0], col_sem.at[1], device_id={"col": 1}, device_id_type=MESH)

    def corn_copy():
        return pltpu.make_async_remote_copy(img_hbm.at[:, 7, pl.ds(120, 8)], corn, corn_sem.at[0], corn_sem.at[1], device_id={"col": 1, "row": row + 1}, device_id_type=MESH)

    def y_place(half, xs, cs):
        return y1v.at[half, pl.ds(1 + 4 * xs, 4), pl.ds(pl.multiple_of(HALF * cs, HALF), HALF)]

    def y_copy(step, i):
        half = step // 4
        return pltpu.make_async_remote_copy(ybuf.at[step, i], y_place(half, x, col), y_send.at[step * 2 + i], y_recv.at[half * 8 + 2 * x + col], device_id={"col": i, "row": base_row + group_of(step, x)}, device_id_type=MESH)

    def y_local(half):
        return pltpu.make_async_copy(ybuf.at[4 * half + 2, col], y_place(half, x, col), self_sem.at[half])

    def ring(src, dst, send, recv, delta):
        return pltpu.make_async_remote_copy(src, dst, send, recv, device_id={"row": row + delta}, device_id_type=MESH)

    def halo1_down(i):
        return ring(y1v.at[i, 16], y1v.at[i, 0], ha_s.at[i], ha_r.at[i], 4)

    def halo1_up(i):
        return ring(y1v.at[i, 1], y1v.at[i, 17], ha_s.at[2 + i], ha_r.at[2 + i], -4)

    def halo2(i):
        return ring(eo1.at[:, i, 16], eo1.at[:, i, 0], hb_s.at[i], hb_r.at[i], 4)

    def halo3_down(i):
        return ring(y2v.at[i, 8], y2v.at[i, 0], hc_s.at[i], hc_r.at[i], 4)

    def halo3_up(i):
        return ring(y2v.at[i, 1], y2v.at[i, 9], hc_s.at[2 + i], hc_r.at[2 + i], -4)

    def halo4(i):
        return ring(eo2.at[:, i, 8], eo2.at[:, i, 0], hd_s.at[i], hd_r.at[i], 4)

    load(0).start()

    @pl.when(col == 0)
    def _():
        col_copy().start()

    @pl.when(sends_row)
    def _():
        @pl.when(col == 0)
        def _():
            corn_copy().start()

        def body(step):
            halo_copy(step).start()

        loop(8, body)

    @pl.when(col == 0)
    def _():
        colb[...] = jnp.zeros_like(colb)

    @pl.when(jnp.logical_or(col == 0, row == 0))
    def _():
        corn[...] = jnp.zeros_like(corn)

    @pl.when(row == 0)
    def _():
        halo[...] = jnp.zeros_like(halo)

    @pl.when(jnp.logical_not(has_up))
    def _():
        for i in range(2):
            for ref in (y1v, y2v):
                ref[i, 0] = jnp.zeros(ref.shape[2:], BF16)
            for ref in (eo1, eo2):
                ref[:, i, 0] = jnp.zeros((2,) + ref.shape[3:], BF16)
        y3v[:, 0] = jnp.zeros((2, 32, TOP), BF16)

    @pl.when(jnp.logical_not(has_down))
    def _():
        for i in range(2):
            y1v[i, 17] = jnp.zeros(y1v.shape[2:], BF16)
            y2v[i, 9] = jnp.zeros(y2v.shape[2:], BF16)
        y3v[:, 5] = jnp.zeros((2, 32, TOP), BF16)

    @pl.when(col == 1)
    def _():
        col_copy().wait_recv()

        @pl.when(row > 0)
        def _():
            corn_copy().wait_recv()

    def taps(i, q, left, line):
        for h in range(2):
            lanes = slice(LANE * h, LANE * h + LANE)
            frow[h, 0:8] = left[:, lanes].astype(F32)
            frow[h, 8:136] = line[:, lanes].astype(F32)
        for t in range(3):
            for h in range(2):
                xbuf[i, q, :, PART * t + LANE * h : PART * t + LANE * h + LANE] = frow[h, pl.ds(7 + t, HALF, stride=2)].astype(BF16)

    def is_local(step, i):
        return jnp.logical_and(lax.rem(step, 4) == 2, col == i)

    def stage_d1(step):
        slot = lax.rem(step, 2)
        first = image_of(step, x)

        @pl.when(step < 7)
        def _():
            load(step + 1).start()

        for n in range(3):
            @pl.when(step == n + 1)
            def _(n=n):
                weights_start(n)

        load(step).wait()

        @pl.when(row > 0)
        def _():
            halo_copy(step).wait_recv()

        for i in range(2):
            taps(i, 0, corn[first + i], halo[step, i])

            def line(q, i=i):
                taps(i, q + 1, colb[first + i, q], inb[slot, i, q])

            loop(8, line)
        acc = None
        for dy in range(3):
            lhs = jnp.concatenate([xbuf[i, 2 * o + dy] for i in range(2) for o in range(4)], axis=0)
            part = jnp.dot(lhs, w0_ref[dy], preferred_element_type=F32)
            acc = part if acc is None else acc + part
        out = jnp.maximum(acc + b0_ref[...], 0.0).astype(BF16)
        ybuf[step] = out.reshape(2, 4, HALF, WIDE)
        for i in range(2):
            here = is_local(step, i)

            @pl.when(here)
            def _():
                y_local(step // 4).start()

            @pl.when(jnp.logical_not(here))
            def _(i=i):
                y_copy(step, i).start()

    loop(8, stage_d1)

    def tap(base, size, dy, dx, n):
        first = base + (n // 2) * 9 * size + (3 * dy + dx) * size
        return wbuf[pl.ds(first, size), :, lanes_of(lax.rem(n, 2))].reshape(WIDE * size, PART)

    def refine_block(src, i, first, rows, base, size, n):
        width = src.shape[2]
        m = rows * width
        lhs = jnp.concatenate([src[i, pl.ds(first + dy, rows)].reshape(m, -1) for dy in range(3)], axis=1)
        parts = []
        for dx in range(3):
            rhs = jnp.concatenate([tap(base, size, dy, dx, n) for dy in range(3)], axis=0)
            parts.append(jnp.dot(lhs, rhs, preferred_element_type=F32))
        return parts[1] + shifted(parts[0], 1, width) + shifted(parts[2], -1, width)

    def lanes_of(n):
        return pl.ds(pl.multiple_of(n * PART, PART), PART)

    def stage_r1(i):
        def piece(step):
            block = lax.rem(1 + step, 4)

            @pl.when(block == 3)
            def _():
                @pl.when(has_down)
                def _():
                    halo1_up(i).wait_recv()

                @pl.when(has_up)
                def _():
                    halo1_down(i).wait_recv()

            def chunk(n):
                lanes = lanes_of(n)
                out = refine_block(y1v, i, 4 * block, 4, 0, 1, n)
                out = jnp.maximum(out + b1_ref[:, lanes], 0.0)
                split_columns(out, scratch, eo1.at[0], eo1.at[1], (i, pl.ds(1 + 4 * block, 4)), n * PART, 4, LANE)

            loop(2, chunk)

            @pl.when(jnp.logical_and(has_down, block == 3))
            def _():
                halo2(i).start()

        loop(4, piece)

    def stage_d2(i):
        @pl.when(has_up)
        def _():
            halo2(i).wait_recv()

        def chunk(n):
            lanes = lanes_of(n)

            def gather(ref):
                return [jnp.concatenate([eo1[ref, i, 2 * o + dy] for o in range(8)], axis=0) for dy in range(3)]

            odd = gather(1)
            both = jnp.concatenate(gather(0) + odd, axis=1)
            rhs = jnp.concatenate([tap(9, 1, dy, dx, n) for dx in (1, 2) for dy in range(3)], axis=0)
            left = jnp.concatenate([tap(9, 1, dy, 0, n) for dy in range(3)], axis=0)
            out = jnp.dot(both, rhs, preferred_element_type=F32)
            out = out + shifted(jnp.dot(jnp.concatenate(odd, axis=1), left, preferred_element_type=F32), 1, HALF)
            out = jnp.maximum(out + b2_ref[:, lanes], 0.0).astype(BF16)
            y2v[i, 1:9, :, lanes] = out.reshape(8, HALF, PART)

        loop(4, chunk)

        @pl.when(has_down)
        def _():
            halo3_down(i).start()

        @pl.when(has_up)
        def _():
            halo3_up(i).start()

    def halo3_wait(i):
        @pl.when(has_up)
        def _():
            halo3_down(i).wait_recv()

        @pl.when(has_down)
        def _():
            halo3_up(i).wait_recv()

    def stage_r2(i, begin, count, top, rows):
        def chunk(step):
            n = begin + step
            lanes = lanes_of(n)
            out = refine_block(y2v, i, top, rows, 27, 2, n)
            out = jnp.maximum(out + b3_ref[:, lanes], 0.0)
            split_columns(out, scratch, eo2.at[0], eo2.at[1], (i, pl.ds(1 + top, rows)), n * PART, rows, HALF)

        loop(count, chunk)

    def halo4_start(i):
        @pl.when(has_down)
        def _():
            halo4(i).start()

    def per_image(half):
        y_local(half).wait()
        for xs in range(4):
            for cs in range(2):
                @pl.when(jnp.logical_or(xs != x, cs != col))
                def _(xs=xs, cs=cs):
                    pltpu.make_async_remote_copy(ybuf.at[0, 0], y_place(half, xs, cs), y_send.at[0], y_recv.at[half * 8 + 2 * xs + cs], device_id={"col": cs, "row": base_row + xs}, device_id_type=MESH).wait_recv()

        @pl.when(has_down)
        def _():
            halo1_down(half).start()

        @pl.when(has_up)
        def _():
            halo1_up(half).start()

        @pl.when(half == 0)
        def _():
            weights_wait(0)

        stage_r1(half)

        @pl.when(half == 0)
        def _():
            weights_wait(1)

        stage_d2(half)

        @pl.when(half == 0)
        def _():
            halo3_wait(0)
            weights_wait(2)

        @pl.when(half == 1)
        def _():
            for t in range(4):
                start_all(load4(t))

        stage_r2(0, 2 * half, 2, 0, 8)

    loop(2, per_image)
    halo4_start(0)
    halo3_wait(1)
    stage_r2(1, 0, 4, 4, 4)
    halo4_start(1)
    stage_r2(1, 0, 4, 0, 4)

    @pl.when(has_up)
    def _():
        for i in range(2):
            halo4(i).wait_recv()

    def halo_up(n):
        return pltpu.make_async_remote_copy(y3v.at[:, 1, :, wide(n)], y3v.at[:, 5, :, wide(n)], up_s.at[n], up_r.at[n], device_id={"row": row - 4}, device_id_type=MESH)

    def halo_down(n):
        return pltpu.make_async_remote_copy(y3v.at[:, 4, :, wide(n)], y3v.at[:, 0, :, wide(n)], down_s.at[n], down_r.at[n], device_id={"row": row + 4}, device_id_type=MESH)

    def out_copy(n, xd, cd):
        dst = out_hbm.at[x, :, col, :, wide(n)]
        return pltpu.make_async_remote_copy(ybuf.at[n, :, xd, pl.ds(16 * cd, 16)], dst, o_s.at[n, 2 * xd + cd], o_r.at[n, 2 * x + col], device_id={"col": cd, "row": base_row + xd}, device_id_type=MESH)

    def out_recv(n, xs, cs):
        dst = out_hbm.at[xs, :, cs, :, wide(n)]
        return pltpu.make_async_remote_copy(ybuf.at[n, :, xs, pl.ds(16 * cs, 16)], dst, o_s.at[n, 2 * xs + cs], o_r.at[n, 2 * xs + cs], device_id={"col": cs, "row": base_row + xs}, device_id_type=MESH)

    def out_self(n):
        dst = out_hbm.at[x, :, col, :, wide(n)]
        return pltpu.make_async_copy(ybuf.at[n, :, x, pl.ds(pl.multiple_of(16 * col, 16), 16)], dst, out_sem.at[n])

    def stage_d3(t):
        wait_all(load4(t))
        ahead = t + 3

        @pl.when(jnp.logical_and(t >= 1, ahead < total))
        def _():
            start_all(load4(ahead))

        for k in range(3):
            @pl.when(t == 3 + 2 * k)
            def _(k=k):
                start_all(load5(k))

        j = lax.rem(t, 3)
        n = t // 3
        plane_index = (j + 1) // 2
        lhs = jnp.concatenate([jnp.concatenate([eo2[plane_index, i, 2 * o + dy] for i in range(2) for o in range(4)], axis=0) for dy in range(3)], axis=1)
        rhs = wbuf[pl.ds(6 * lax.rem(t, 4), 6)].reshape(3072, WIDE)
        acc[j] = jnp.dot(lhs, rhs, preferred_element_type=F32)

        @pl.when(j == 2)
        def _():
            out = acc[0] + acc[1] + shifted(acc[2], 1, 32)
            out = jnp.maximum(out + b4_ref[:, wide(n)], 0.0).astype(BF16)
            y3v[:, 1:5, :, wide(n)] = out.reshape(2, 4, 32, WIDE)

            @pl.when(has_up)
            def _():
                halo_up(n).start()

            @pl.when(has_down)
            def _():
                halo_down(n).start()

    loop(total, stage_d3)
    for t in (3, 4):
        start_all(load5(t))

    def finish(step):
        for i in range(2):
            @pl.when(jnp.logical_not(is_local(step, i)))
            def _(i=i):
                y_copy(step, i).wait_send()

        @pl.when(sends_row)
        def _():
            halo_copy(step).wait_send()

    loop(8, finish)

    def halo_wait(n):
        @pl.when(has_down)
        def _():
            halo_up(n).wait_recv()

        @pl.when(has_up)
        def _():
            halo_down(n).wait_recv()

    loop(total // 3, halo_wait)

    def stage_r3(t):
        wait_all(load5(t))
        ahead = t + 4

        @pl.when(jnp.logical_and(t >= 1, ahead < total))
        def _():
            start_all(load5(ahead))

        j = lax.rem(t, 3)
        n = t // 3
        lhs = jnp.concatenate([y3v[:, dy : dy + 4].reshape(PART, TOP) for dy in range(3)], axis=1)
        rhs = wbuf[pl.ds(base5(t), 12)].reshape(6144, WIDE)
        acc[j] = jnp.dot(lhs, rhs, preferred_element_type=F32)

        @pl.when(j == 2)
        def _():
            out = acc[0] + shifted(acc[1], -1, 32) + shifted(acc[2], 1, 32)
            out = jnp.maximum(out + b5_ref[:, wide(n)], 0.0).astype(BF16)
            ybuf[n, :, :, 0:32] = out.reshape(2, 4, 32, WIDE)
            for xd in range(4):
                for cd in range(2):
                    here = jnp.logical_and(x == xd, col == cd)

                    @pl.when(here)
                    def _():
                        out_self(n).start()

                    @pl.when(jnp.logical_not(here))
                    def _(xd=xd, cd=cd):
                        out_copy(n, xd, cd).start()

    loop(total, stage_r3)

    def finish_out(n):
        out_self(n).wait()
        for xd in range(4):
            for cd in range(2):
                @pl.when(jnp.logical_or(x != xd, col != cd))
                def _(xd=xd, cd=cd):
                    out_copy(n, xd, cd).wait_send()
                    out_recv(n, xd, cd).wait_recv()

        @pl.when(has_up)
        def _():
            halo_up(n).wait_send()

        @pl.when(has_down)
        def _():
            halo_down(n).wait_send()

    loop(total // 3, finish_out)


    @pl.when(col == 0)
    def _():
        col_copy().wait_send()

        @pl.when(sends_row)
        def _():
            corn_copy().wait_send()

    @pl.when(has_down)
    def _():
        for i in range(2):
            halo1_down(i).wait_send()
            halo3_down(i).wait_send()
            halo2(i).wait_send()
            halo4(i).wait_send()

    @pl.when(has_up)
    def _():
        for i in range(2):
            halo1_up(i).wait_send()
            halo3_up(i).wait_send()


def encoder(row_size, images, weights, biases):
    def kernel(*refs):
        encoder_kernel(row_size, *refs)

    w0, w1, w2, w3, w4, w5 = weights
    flat = [b.reshape(1, -1) for b in biases]
    return pl.pallas_call(
        kernel,
        out_shape=jax.ShapeDtypeStruct((4, 2, 2, 16, TOP), BF16),
        in_specs=[ANY_SPEC, VM_SPEC, VM_SPEC] + [ANY_SPEC] * 5 + [VM_SPEC] * 5,
        out_specs=ANY_SPEC,
        scratch_shapes=[
            VM((2, 2, 8, LANE, PART), BF16),
            VM((8, 2, LANE, PART), BF16),
            VM((16, 8, 8, PART), BF16),
            VM((16, 8, PART), BF16),
            VM((2, 136, LANE), F32),
            VM((2, 9, HALF, 768), BF16),
            VM((8, 2, 4, HALF, WIDE), BF16),
            VM((2, 18, LANE, WIDE), BF16),
            VM((63, WIDE, WIDE), BF16),
            VM((2, 2, 17, HALF, WIDE), BF16),
            VM((2, 10, HALF, MID), BF16),
            VM((2, WIDE, LANE), F32),
            VM((2, 2, 9, 32, MID), BF16),
            VM((2, 6, 32, TOP), BF16),
            VM((3, PART, WIDE), F32),
        ]
        + [SEM((n,)) for n in (2, 8, 8, 2, 2, 16, 16, 2, 5)]
        + [SEM((4,))] * 13
        + [SEM(n) for n in ((4, 3), (5, 3), (4, 8), (4, 8))],
        compiler_params=PARAMS,
        name="encoder",
    )(images, w0.reshape(3, 768, WIDE), flat[0], w1.reshape(9, WIDE, WIDE), w2.reshape(9, WIDE, MID), w3.reshape(18, WIDE, MID), w4.reshape(3, 3, 2, WIDE, TOP), w5.reshape(3, 3, 4, WIDE, TOP), *flat[1:])


def solution(mesh):
    row_size = mesh.shape["row"]

    def local_encoder(images, w_down1, b_down1, w_refine1, b_refine1, w_down2, b_down2, w_refine2, b_refine2, w_down3, b_down3, w_refine3, b_refine3):
        weights = (w_down1, w_refine1, w_down2, w_refine2, w_down3, w_refine3)
        biases = (b_down1, b_refine1, b_down2, b_refine2, b_down3, b_refine3)
        return encoder(row_size, images, weights, biases).reshape(16, 1, 16, TOP)

    tile_spec = P("dp", "row", "col")
    return jax.shard_map(local_encoder, mesh=mesh, in_specs=(tile_spec,) + (P(),) * 12, out_specs=tile_spec, check_vma=False)
```

```python
import jax
import jax.numpy as jnp
from jax import lax
from jax.experimental import pallas as pl
from jax.experimental.pallas import tpu as pltpu
from jax.sharding import PartitionSpec as P

MESH = pl.DeviceIdType.MESH
BF16 = jnp.bfloat16
F32 = jnp.float32
WIDE = 512
TOP = 2048
MID = 1024
PART = 256
LANE = 128
HALF = 64
VM = pltpu.VMEM
SEM = pltpu.SemaphoreType.DMA
ANY_SPEC = pl.BlockSpec(memory_space=pl.ANY)
VM_SPEC = pl.BlockSpec(memory_space=VM)
PARAMS = pltpu.CompilerParams(has_side_effects=True, vmem_limit_bytes=67043328)


def loop(count, fn):
    def body(step, carry):
        fn(step)
        return carry

    lax.fori_loop(0, count, body, 0)


def shifted(value, by, width):
    size = value.shape[0]
    pos = lax.rem(lax.broadcasted_iota(jnp.int32, (size, 1), 0), width)
    edge = 0 if by == 1 else width - 1
    return jnp.where(pos == edge, 0.0, pltpu.roll(value, by % size, 0))


def split_columns(value, scratch, even_ref, odd_ref, index, lane, rows, width):
    half = width // 2
    for h in range(2):
        scratch[h, 0 : rows * width] = value[:, LANE * h : LANE * h + LANE]
        lanes = pl.ds(pl.multiple_of(lane + LANE * h, LANE), LANE)
        for ref, start in ((even_ref, 0), (odd_ref, 1)):
            part = scratch[h, pl.ds(start, rows * half, stride=2)].astype(BF16)
            ref[index[0], index[1], :, lanes] = part.reshape(rows, half, LANE)


def encoder_kernel(row_size, img_hbm, w0_hbm, b0_ref, w1_hbm, w2_hbm, w3_hbm, w4_hbm, w5_hbm, b1_ref, b2_ref, b3_ref, b4_ref, b5_ref, out_hbm, inb, halo, colb, corn, frow, xbuf, ybuf, y1v, wbuf, eo1, y2v, scratch, eo2, y3v, acc, in_sem, halo_send, halo_recv, col_sem, corn_sem, y_send, y_recv, self_sem, w_sem, ha_s, ha_r, hb_s, hb_r, hc_s, hc_r, hd_s, hd_r, up_s, up_r, down_s, down_r, out_sem, w4_sem, w5_sem, o_s, o_r):
    col = lax.axis_index("col")
    row = lax.axis_index("row")
    x = lax.rem(row, 4)
    base_row = row - x
    has_up = row >= 4
    has_down = row < row_size - 4
    sends_row = row < row_size - 1
    total = 3 * (TOP // WIDE)

    def plane(src, part, first, count, n):
        return pltpu.make_async_copy(src.at[:, :, pl.ds(WIDE * part, WIDE)], wbuf.at[pl.ds(first, count)], w_sem.at[n])

    weights = [[plane(w1_hbm, 0, 0, 9, 0)], [plane(w2_hbm, k, 9 + 9 * k, 9, 1 + k) for k in range(2)], [plane(w3_hbm, k, 27 + 18 * k, 18, 3 + k) for k in range(2)]]

    first_copy = pltpu.make_async_copy(w0_hbm, wbuf.at[pl.ds(27, 9), pl.ds(0, PART)], w_sem.at[5])

    def weights_start(n):
        for copy in weights[n]:
            copy.start()

    def weights_wait(n):
        for copy in weights[n]:
            copy.wait()

    def wide(n):
        return pl.ds(pl.multiple_of(n * WIDE, WIDE), WIDE)

    def load4(t):
        slot = lax.rem(t, 4)
        return [pltpu.make_async_copy(w4_hbm.at[dy, lax.rem(t + 1, 3), :, :, wide(t // 3)], wbuf.at[pl.ds(6 * slot + 2 * dy, 2)], w4_sem.at[slot, dy]) for dy in range(3)]

    def base5(t):
        return lax.rem(27 + 12 * lax.rem(t, 5), 63)

    def load5(t):
        return [pltpu.make_async_copy(w5_hbm.at[dy, lax.rem(t + 1, 3), :, :, wide(t // 3)], wbuf.at[pl.ds(base5(t) + 4 * dy, 4)], w5_sem.at[lax.rem(t, 5), dy]) for dy in range(3)]

    def start_all(copies):
        for copy in copies:
            copy.start()

    def wait_all(copies):
        for copy in copies:
            copy.wait()

    def group_of(step, xpos):
        turn = lax.rem(step, 4)
        turn = jnp.where(turn < 2, turn + col * (1 - 2 * turn), turn)
        return lax.rem(xpos + 6 - turn, 4)

    def image_of(step, xpos):
        return 4 * group_of(step, xpos) + 2 * (step // 4)

    def load(step):
        slot = lax.rem(step, 2)
        return pltpu.make_async_copy(img_hbm.at[pl.ds(image_of(step, x), 2)], inb.at[slot], in_sem.at[slot])

    def halo_copy(step):
        first = image_of(step, lax.rem(x + 1, 4))
        return pltpu.make_async_remote_copy(img_hbm.at[pl.ds(first, 2), 7], halo.at[step], halo_send.at[step], halo_recv.at[step], device_id={"row": row + 1}, device_id_type=MESH)

    def col_copy():
        return pltpu.make_async_remote_copy(img_hbm.at[:, :, pl.ds(120, 8)], colb, col_sem.at[0], col_sem.at[1], device_id={"col": 1}, device_id_type=MESH)

    def corn_copy():
        return pltpu.make_async_remote_copy(img_hbm.at[:, 7, pl.ds(120, 8)], corn, corn_sem.at[0], corn_sem.at[1], device_id={"col": 1, "row": row + 1}, device_id_type=MESH)

    def y_place(half, xs, cs):
        return y1v.at[half, pl.ds(1 + 4 * xs, 4), pl.ds(pl.multiple_of(HALF * cs, HALF), HALF)]

    def y_copy(step, i):
        half = step // 4
        return pltpu.make_async_remote_copy(ybuf.at[step, i], y_place(half, x, col), y_send.at[step * 2 + i], y_recv.at[half * 8 + 2 * x + col], device_id={"col": i, "row": base_row + group_of(step, x)}, device_id_type=MESH)

    def y_local(half):
        return pltpu.make_async_copy(ybuf.at[4 * half + 2, col], y_place(half, x, col), self_sem.at[half])

    def ring(src, dst, send, recv, delta):
        return pltpu.make_async_remote_copy(src, dst, send, recv, device_id={"row": row + delta}, device_id_type=MESH)

    def halo1_down(i):
        return ring(y1v.at[i, 16], y1v.at[i, 0], ha_s.at[i], ha_r.at[i], 4)

    def halo1_up(i):
        return ring(y1v.at[i, 1], y1v.at[i, 17], ha_s.at[2 + i], ha_r.at[2 + i], -4)

    def halo2(i):
        return ring(eo1.at[:, i, 16], eo1.at[:, i, 0], hb_s.at[i], hb_r.at[i], 4)

    def halo3_down(i):
        return ring(y2v.at[i, 8], y2v.at[i, 0], hc_s.at[i], hc_r.at[i], 4)

    def halo3_up(i):
        return ring(y2v.at[i, 1], y2v.at[i, 9], hc_s.at[2 + i], hc_r.at[2 + i], -4)

    def halo4(i):
        return ring(eo2.at[:, i, 8], eo2.at[:, i, 0], hd_s.at[i], hd_r.at[i], 4)

    first_copy.start()
    load(0).start()

    @pl.when(col == 0)
    def _():
        col_copy().start()

    @pl.when(sends_row)
    def _():
        @pl.when(col == 0)
        def _():
            corn_copy().start()

        def body(step):
            halo_copy(step).start()

        loop(8, body)

    @pl.when(col == 0)
    def _():
        colb[...] = jnp.zeros_like(colb)

    @pl.when(jnp.logical_or(col == 0, row == 0))
    def _():
        corn[...] = jnp.zeros_like(corn)

    @pl.when(row == 0)
    def _():
        halo[...] = jnp.zeros_like(halo)

    @pl.when(jnp.logical_not(has_up))
    def _():
        for i in range(2):
            for ref in (y1v, y2v):
                ref[i, 0] = jnp.zeros(ref.shape[2:], BF16)
            for ref in (eo1, eo2):
                ref[:, i, 0] = jnp.zeros((2,) + ref.shape[3:], BF16)
        y3v[:, 0] = jnp.zeros((2, 32, TOP), BF16)

    @pl.when(jnp.logical_not(has_down))
    def _():
        for i in range(2):
            y1v[i, 17] = jnp.zeros(y1v.shape[2:], BF16)
            y2v[i, 9] = jnp.zeros(y2v.shape[2:], BF16)
        y3v[:, 5] = jnp.zeros((2, 32, TOP), BF16)

    @pl.when(col == 1)
    def _():
        col_copy().wait_recv()

        @pl.when(row > 0)
        def _():
            corn_copy().wait_recv()

    def taps(i, q, left, line):
        for h in range(2):
            lanes = slice(LANE * h, LANE * h + LANE)
            frow[h, 0:8] = left[:, lanes].astype(F32)
            frow[h, 8:136] = line[:, lanes].astype(F32)
        for t in range(3):
            for h in range(2):
                xbuf[i, q, :, PART * t + LANE * h : PART * t + LANE * h + LANE] = frow[h, pl.ds(7 + t, HALF, stride=2)].astype(BF16)

    def is_local(step, i):
        return jnp.logical_and(lax.rem(step, 4) == 2, col == i)

    def stage_d1(step):
        slot = lax.rem(step, 2)
        first = image_of(step, x)

        @pl.when(step < 7)
        def _():
            load(step + 1).start()

        for n in range(2):
            @pl.when(step == n + 1)
            def _(n=n):
                weights_start(n)

        load(step).wait()

        @pl.when(row > 0)
        def _():
            halo_copy(step).wait_recv()

        for i in range(2):
            taps(i, 0, corn[first + i], halo[step, i])

            def line(q, i=i):
                taps(i, q + 1, colb[first + i, q], inb[slot, i, q])

            loop(8, line)
        acc = None
        for dy in range(3):
            lhs = jnp.concatenate([xbuf[i, 2 * o + dy] for i in range(2) for o in range(4)], axis=0)
            rhs = wbuf[27 + 3 * dy : 30 + 3 * dy, 0:PART].reshape(768, WIDE)
            part = jnp.dot(lhs, rhs, preferred_element_type=F32)
            acc = part if acc is None else acc + part
        out = jnp.maximum(acc + b0_ref[...], 0.0).astype(BF16)
        ybuf[step] = out.reshape(2, 4, HALF, WIDE)
        for i in range(2):
            here = is_local(step, i)

            @pl.when(here)
            def _():
                y_local(step // 4).start()

            @pl.when(jnp.logical_not(here))
            def _(i=i):
                y_copy(step, i).start()

    first_copy.wait()
    loop(8, stage_d1)
    weights_start(2)

    def tap(base, size, dy, dx, n):
        first = base + (n // 2) * 9 * size + (3 * dy + dx) * size
        return wbuf[pl.ds(first, size), :, lanes_of(lax.rem(n, 2))].reshape(WIDE * size, PART)

    def refine_block(src, i, first, rows, base, size, n):
        width = src.shape[2]
        m = rows * width
        lhs = jnp.concatenate([src[i, pl.ds(first + dy, rows)].reshape(m, -1) for dy in range(3)], axis=1)
        parts = []
        for dx in range(3):
            rhs = jnp.concatenate([tap(base, size, dy, dx, n) for dy in range(3)], axis=0)
            parts.append(jnp.dot(lhs, rhs, preferred_element_type=F32))
        return parts[1] + shifted(parts[0], 1, width) + shifted(parts[2], -1, width)

    def lanes_of(n):
        return pl.ds(pl.multiple_of(n * PART, PART), PART)

    def stage_r1(i):
        def piece(step):
            block = lax.rem(1 + step, 4)

            @pl.when(block == 3)
            def _():
                @pl.when(has_down)
                def _():
                    halo1_up(i).wait_recv()

                @pl.when(has_up)
                def _():
                    halo1_down(i).wait_recv()

            def chunk(n):
                lanes = lanes_of(n)
                out = refine_block(y1v, i, 4 * block, 4, 0, 1, n)
                out = jnp.maximum(out + b1_ref[:, lanes], 0.0)
                split_columns(out, scratch, eo1.at[0], eo1.at[1], (i, pl.ds(1 + 4 * block, 4)), n * PART, 4, LANE)

            loop(2, chunk)

            @pl.when(jnp.logical_and(has_down, block == 3))
            def _():
                halo2(i).start()

        loop(4, piece)

    def stage_d2(i):
        @pl.when(has_up)
        def _():
            halo2(i).wait_recv()

        def chunk(n):
            lanes = lanes_of(n)

            def gather(ref):
                return [jnp.concatenate([eo1[ref, i, 2 * o + dy] for o in range(8)], axis=0) for dy in range(3)]

            odd = gather(1)
            both = jnp.concatenate(gather(0) + odd, axis=1)
            rhs = jnp.concatenate([tap(9, 1, dy, dx, n) for dx in (1, 2) for dy in range(3)], axis=0)
            left = jnp.concatenate([tap(9, 1, dy, 0, n) for dy in range(3)], axis=0)
            out = jnp.dot(both, rhs, preferred_element_type=F32)
            out = out + shifted(jnp.dot(jnp.concatenate(odd, axis=1), left, preferred_element_type=F32), 1, HALF)
            out = jnp.maximum(out + b2_ref[:, lanes], 0.0).astype(BF16)
            y2v[i, 1:9, :, lanes] = out.reshape(8, HALF, PART)

        loop(4, chunk)

        @pl.when(has_down)
        def _():
            halo3_down(i).start()

        @pl.when(has_up)
        def _():
            halo3_up(i).start()

    def halo3_wait(i):
        @pl.when(has_up)
        def _():
            halo3_down(i).wait_recv()

        @pl.when(has_down)
        def _():
            halo3_up(i).wait_recv()

    def stage_r2(i, begin, count, top, rows):
        def chunk(step):
            n = begin + step
            lanes = lanes_of(n)
            out = refine_block(y2v, i, top, rows, 27, 2, n)
            out = jnp.maximum(out + b3_ref[:, lanes], 0.0)
            split_columns(out, scratch, eo2.at[0], eo2.at[1], (i, pl.ds(1 + top, rows)), n * PART, rows, HALF)

        loop(count, chunk)

    def halo4_start(i):
        @pl.when(has_down)
        def _():
            halo4(i).start()

    def per_image(half):
        y_local(half).wait()
        for xs in range(4):
            for cs in range(2):
                @pl.when(jnp.logical_or(xs != x, cs != col))
                def _(xs=xs, cs=cs):
                    pltpu.make_async_remote_copy(ybuf.at[0, 0], y_place(half, xs, cs), y_send.at[0], y_recv.at[half * 8 + 2 * xs + cs], device_id={"col": cs, "row": base_row + xs}, device_id_type=MESH).wait_recv()

        @pl.when(has_down)
        def _():
            halo1_down(half).start()

        @pl.when(has_up)
        def _():
            halo1_up(half).start()

        @pl.when(half == 0)
        def _():
            weights_wait(0)

        stage_r1(half)

        @pl.when(half == 0)
        def _():
            weights_wait(1)

        stage_d2(half)

        @pl.when(half == 1)
        def _():
            for t in range(4):
                start_all(load4(t))


    loop(2, per_image)
    halo3_wait(0)
    weights_wait(2)
    stage_r2(0, 0, 4, 0, 8)
    halo4_start(0)
    halo3_wait(1)
    stage_r2(1, 0, 4, 4, 4)
    halo4_start(1)
    stage_r2(1, 0, 4, 0, 4)

    @pl.when(has_up)
    def _():
        for i in range(2):
            halo4(i).wait_recv()

    def halo_up(n):
        return pltpu.make_async_remote_copy(y3v.at[:, 1, :, wide(n)], y3v.at[:, 5, :, wide(n)], up_s.at[n], up_r.at[n], device_id={"row": row - 4}, device_id_type=MESH)

    def halo_down(n):
        return pltpu.make_async_remote_copy(y3v.at[:, 4, :, wide(n)], y3v.at[:, 0, :, wide(n)], down_s.at[n], down_r.at[n], device_id={"row": row + 4}, device_id_type=MESH)

    def out_copy(n, xd, cd):
        dst = out_hbm.at[x, :, col, :, wide(n)]
        return pltpu.make_async_remote_copy(ybuf.at[n, :, xd, pl.ds(16 * cd, 16)], dst, o_s.at[n, 2 * xd + cd], o_r.at[n, 2 * x + col], device_id={"col": cd, "row": base_row + xd}, device_id_type=MESH)

    def out_recv(n, xs, cs):
        dst = out_hbm.at[xs, :, cs, :, wide(n)]
        return pltpu.make_async_remote_copy(ybuf.at[n, :, xs, pl.ds(16 * cs, 16)], dst, o_s.at[n, 2 * xs + cs], o_r.at[n, 2 * xs + cs], device_id={"col": cs, "row": base_row + xs}, device_id_type=MESH)

    def out_self(n):
        dst = out_hbm.at[x, :, col, :, wide(n)]
        return pltpu.make_async_copy(ybuf.at[n, :, x, pl.ds(pl.multiple_of(16 * col, 16), 16)], dst, out_sem.at[n])

    def stage_d3(t):
        wait_all(load4(t))
        ahead = t + 3

        @pl.when(jnp.logical_and(t >= 1, ahead < total))
        def _():
            start_all(load4(ahead))

        for k in range(3):
            @pl.when(t == 3 + 2 * k)
            def _(k=k):
                start_all(load5(k))

        j = lax.rem(t, 3)
        n = t // 3
        plane_index = (j + 1) // 2
        lhs = jnp.concatenate([jnp.concatenate([eo2[plane_index, i, 2 * o + dy] for i in range(2) for o in range(4)], axis=0) for dy in range(3)], axis=1)
        rhs = wbuf[pl.ds(6 * lax.rem(t, 4), 6)].reshape(3072, WIDE)
        acc[j] = jnp.dot(lhs, rhs, preferred_element_type=F32)

        @pl.when(j == 2)
        def _():
            out = acc[0] + acc[1] + shifted(acc[2], 1, 32)
            out = jnp.maximum(out + b4_ref[:, wide(n)], 0.0).astype(BF16)
            y3v[:, 1:5, :, wide(n)] = out.reshape(2, 4, 32, WIDE)

            @pl.when(has_up)
            def _():
                halo_up(n).start()

            @pl.when(has_down)
            def _():
                halo_down(n).start()

    loop(total, stage_d3)
    for t in (3, 4):
        start_all(load5(t))

    def center_r3(t):
        wait_all(load5(t))
        lhs = y3v[:, 1:5].reshape(PART, TOP)
        acc[t] = jnp.dot(lhs, wbuf[pl.ds(base5(t) + 4, 4)].reshape(TOP, WIDE), preferred_element_type=F32)

    loop(3, center_r3)

    def finish(step):
        for i in range(2):
            @pl.when(jnp.logical_not(is_local(step, i)))
            def _(i=i):
                y_copy(step, i).wait_send()

        @pl.when(sends_row)
        def _():
            halo_copy(step).wait_send()

    loop(8, finish)

    def halo_wait(n):
        @pl.when(has_down)
        def _():
            halo_up(n).wait_recv()

        @pl.when(has_up)
        def _():
            halo_down(n).wait_recv()

    loop(total // 3, halo_wait)

    def stage_r3(t):
        @pl.when(t >= 3)
        def _():
            wait_all(load5(t))

        ahead = t + 4

        @pl.when(jnp.logical_and(t >= 1, ahead < total))
        def _():
            start_all(load5(ahead))

        j = lax.rem(t, 3)
        n = t // 3

        def rows_of(dy):
            return y3v[:, dy : dy + 4].reshape(PART, TOP)

        @pl.when(t < 3)
        def _():
            lhs = jnp.concatenate([rows_of(0), rows_of(2)], axis=1)
            rhs = jnp.concatenate([wbuf[pl.ds(base5(t) + 8 * k, 4)].reshape(TOP, WIDE) for k in range(2)], axis=0)
            acc[j] += jnp.dot(lhs, rhs, preferred_element_type=F32)

        @pl.when(t >= 3)
        def _():
            lhs = jnp.concatenate([rows_of(dy) for dy in range(3)], axis=1)
            rhs = wbuf[pl.ds(base5(t), 12)].reshape(6144, WIDE)
            acc[j] = jnp.dot(lhs, rhs, preferred_element_type=F32)

        @pl.when(j == 2)
        def _():
            out = acc[0] + shifted(acc[1], -1, 32) + shifted(acc[2], 1, 32)
            out = jnp.maximum(out + b5_ref[:, wide(n)], 0.0).astype(BF16)
            ybuf[n, :, :, 0:32] = out.reshape(2, 4, 32, WIDE)
            for xd in range(4):
                for cd in range(2):
                    here = jnp.logical_and(x == xd, col == cd)

                    @pl.when(here)
                    def _():
                        out_self(n).start()

                    @pl.when(jnp.logical_not(here))
                    def _(xd=xd, cd=cd):
                        out_copy(n, xd, cd).start()

    loop(total, stage_r3)

    def finish_out(n):
        out_self(n).wait()
        for xd in range(4):
            for cd in range(2):
                @pl.when(jnp.logical_or(x != xd, col != cd))
                def _(xd=xd, cd=cd):
                    out_copy(n, xd, cd).wait_send()
                    out_recv(n, xd, cd).wait_recv()

        @pl.when(has_up)
        def _():
            halo_up(n).wait_send()

        @pl.when(has_down)
        def _():
            halo_down(n).wait_send()

    loop(total // 3, finish_out)


    @pl.when(col == 0)
    def _():
        col_copy().wait_send()

        @pl.when(sends_row)
        def _():
            corn_copy().wait_send()

    @pl.when(has_down)
    def _():
        for i in range(2):
            halo1_down(i).wait_send()
            halo3_down(i).wait_send()
            halo2(i).wait_send()
            halo4(i).wait_send()

    @pl.when(has_up)
    def _():
        for i in range(2):
            halo1_up(i).wait_send()
            halo3_up(i).wait_send()


def encoder(row_size, images, weights, biases):
    def kernel(*refs):
        encoder_kernel(row_size, *refs)

    w0, w1, w2, w3, w4, w5 = weights
    flat = [b.reshape(1, -1) for b in biases]
    return pl.pallas_call(
        kernel,
        out_shape=jax.ShapeDtypeStruct((4, 2, 2, 16, TOP), BF16),
        in_specs=[ANY_SPEC, ANY_SPEC, VM_SPEC] + [ANY_SPEC] * 5 + [VM_SPEC] * 5,
        out_specs=ANY_SPEC,
        scratch_shapes=[
            VM((2, 2, 8, LANE, PART), BF16),
            VM((8, 2, LANE, PART), BF16),
            VM((16, 8, 8, PART), BF16),
            VM((16, 8, PART), BF16),
            VM((2, 136, LANE), F32),
            VM((2, 9, HALF, 768), BF16),
            VM((8, 2, 4, HALF, WIDE), BF16),
            VM((2, 18, LANE, WIDE), BF16),
            VM((63, WIDE, WIDE), BF16),
            VM((2, 2, 17, HALF, WIDE), BF16),
            VM((2, 10, HALF, MID), BF16),
            VM((2, WIDE, LANE), F32),
            VM((2, 2, 9, 32, MID), BF16),
            VM((2, 6, 32, TOP), BF16),
            VM((3, PART, WIDE), F32),
        ]
        + [SEM((n,)) for n in (2, 8, 8, 2, 2, 16, 16, 2, 6)]
        + [SEM((4,))] * 13
        + [SEM(n) for n in ((4, 3), (5, 3), (4, 8), (4, 8))],
        compiler_params=PARAMS,
        name="encoder",
    )(images, w0.reshape(9, PART, WIDE), flat[0], w1.reshape(9, WIDE, WIDE), w2.reshape(9, WIDE, MID), w3.reshape(18, WIDE, MID), w4.reshape(3, 3, 2, WIDE, TOP), w5.reshape(3, 3, 4, WIDE, TOP), *flat[1:])


def solution(mesh):
    row_size = mesh.shape["row"]

    def local_encoder(images, w_down1, b_down1, w_refine1, b_refine1, w_down2, b_down2, w_refine2, b_refine2, w_down3, b_down3, w_refine3, b_refine3):
        weights = (w_down1, w_refine1, w_down2, w_refine2, w_down3, w_refine3)
        biases = (b_down1, b_refine1, b_down2, b_refine2, b_down3, b_refine3)
        return encoder(row_size, images, weights, biases).reshape(16, 1, 16, TOP)

    tile_spec = P("dp", "row", "col")
    return jax.shard_map(local_encoder, mesh=mesh, in_specs=(tile_spec,) + (P(),) * 12, out_specs=tile_spec, check_vma=False)
```
